32 devices in a mesh: rows: 4 (over z), cols: 4 (over x, core), rep: 2 (over y).
Axes of the slice: x: 2, y: 2, z: 4, core: 2. Of those that a mesh axis runs over, the one named last changes fastest.
Arguments:
- matrix: float32 [16384, 8192], P(('rep', 'rows'), 'cols'), parts along dimension 0, may hold values from -0.0625 to 0.0625
- labels: int32 [16384], P(('rep', 'rows')), parts along dimension 0, may hold values from 0 to 1
- lambdas: float32 [64], P('rep'), parts along dimension 0, may hold values from 0.01 to 0.2
- x_prev: float32 [64, 8192], P('rep', 'cols'), parts along dimension 0, may hold values from -4 to 4
- w_prev: float32 [64, 8192], P('rep', 'cols'), parts along dimension 0, may hold values from -4 to 4
- p_prev: float32 [64, 8192], P('rep', 'cols'), parts along dimension 0, may hold values from -1.5 to 1.5
- z_prev: float32 [64, 8192], P('rep', 'rows'), parts along dimension 0, may hold values from -6 to 6
- u_prev: float32 [64, 8192], P('rep', 'rows'), parts along dimension 0, may hold values from -6 to 6
Outputs:
- coeffs: float32 [64, 8192], P('rep', 'cols'), parts along dimension 0
- sparse: float32 [64, 8192], P('rep', 'cols'), parts along dimension 0
- margins: float32 [64, 8192], P('rep', 'rows'), parts along dimension 0
- margin_dual: float32 [64, 8192], P('rep', 'rows'), parts along dimension 0
The draws below stay inside these ranges and needn't reach their ends.
There are 2 independent parts, one for each index of `rep`. The reference program is written for one: setup_inputs(seed, part) draws one part's arguments, and reference() takes and returns one part's arrays. A program takes and returns all parts, laid end to end along the dimension named above; each array names one. Nothing has to cross between parts.
All inputs are finite; a program needn't handle non-finite values.
Results may differ from the reference program's by a relative error of at most 0.0003.
Values sent between devices are 32-bit elements; how exact they have to be, the bound alone decides.
No kernel may reach another device: no remote copies, remote signals or barrier semaphores. Data moves between devices by JAX's collectives and lax.ppermute only.
A program may use at most 128 MiB of HBM per device.

```python
import math
import jax
import jax.numpy as jnp
from jax import lax

FEATURES = 8192
PATHS = 32
ITERS = 2
CG_STEPS = 5
NEWTON_STEPS = 8
SAMPLES = 8192


def touch_ends(result, key, smallest, largest):
    longest = result.shape.index(max(result.shape))
    spots = []
    for shift in (0, 1):
        where = [jax.random.randint(jax.random.fold_in(key, axis), (), 0, length) for axis, length in enumerate(result.shape)]
        where[longest] = (where[longest] + shift) % result.shape[longest]
        spots.append(tuple(where))
    return result.at[spots[0]].set(smallest).at[spots[1]].set(largest)


def shard_levels(stream_key, extent, cuts, least, top_value):
    def one(position, shards_of):
        steps = jax.random.uniform(jax.random.fold_in(jax.random.fold_in(stream_key, 6), position), (shards_of,), jnp.float32, least / len(cuts), top_value / len(cuts))
        return jnp.repeat(jnp.exp(steps), extent[position] // shards_of).reshape((-1,) + (1,) * (len(extent) - position - 1))

    gain = one(*cuts[0])
    for cut in cuts[1:]:
        gain = gain * one(*cut)
    return gain


def gaussian(rng, extent, scale, bound, pieces=(), held_as=jnp.bfloat16):
    loudness = shard_levels(rng, extent, pieces, -0.22, 0.18) if pieces else 1.0
    result = jax.random.normal(rng, extent, jnp.float32) * scale * loudness
    return jnp.minimum(jnp.maximum(result, -bound), bound).astype(held_as)


def setup_inputs(seed: int = 0, part: int = 0) -> dict:
    key_of = jax.random.split(jax.random.key(seed), 9)
    own_keys = jax.random.split(jax.random.fold_in(key_of[8], part), 9)
    matrix = gaussian(own_keys[0], (SAMPLES, FEATURES), FEATURES ** -0.5, 0.0625, ((0, 4), (1, 4)), jnp.float32)
    labels = touch_ends(jax.random.randint(own_keys[1], (SAMPLES,), 0, 2), jax.random.fold_in(own_keys[1], 1), 0, 1).astype(jnp.int32)
    lambdas = jnp.clip(jnp.exp(jax.random.uniform(own_keys[2], (PATHS,), jnp.float32, math.log(0.01), math.log(0.2))), 0.01, 0.2)
    x_prev = gaussian(own_keys[3], (PATHS, FEATURES), 0.3, 4.0, ((1, 4),), jnp.float32)
    w_prev = gaussian(own_keys[4], (PATHS, FEATURES), 0.3, 4.0, ((1, 4),), jnp.float32)
    p_prev = gaussian(own_keys[5], (PATHS, FEATURES), 0.1, 1.5, ((1, 4),), jnp.float32)
    z_prev = gaussian(own_keys[6], (PATHS, SAMPLES), 1.0, 6.0, ((1, 4),), jnp.float32)
    u_prev = gaussian(own_keys[7], (PATHS, SAMPLES), 0.5, 6.0, ((1, 4),), jnp.float32)
    return {"matrix": matrix, "labels": labels, "lambdas": lambdas, "x_prev": x_prev, "w_prev": w_prev, "p_prev": p_prev, "z_prev": z_prev, "u_prev": u_prev}


HIGH = lax.Precision.HIGHEST


def apply_rows(vec, matrix):
    return lax.dot_general(vec, matrix, (((1,), (1,)), ((), ())), precision=HIGH, preferred_element_type=jnp.float32)


def apply_cols(vec, matrix):
    return lax.dot_general(vec, matrix, (((1,), (0,)), ((), ())), precision=HIGH, preferred_element_type=jnp.float32)


def proximal(target, sign):
    margin = target
    for step in range(NEWTON_STEPS):
        grad = margin - target - sign * jax.nn.sigmoid(-sign * margin)
        hess = 1.0 + jax.nn.sigmoid(margin) * jax.nn.sigmoid(-margin)
        margin = margin - grad / hess
    return margin


def reference(matrix, labels, lambdas, x_prev, w_prev, p_prev, z_prev, u_prev):
    sign = 2.0 * labels.astype(jnp.float32) - 1.0
    coeffs, sparse, dual, margins, margin_dual = x_prev, w_prev, p_prev, z_prev, u_prev
    for outer in range(ITERS):
        resid = (sparse - dual - coeffs) + apply_cols(margins - margin_dual - apply_rows(coeffs, matrix), matrix)
        direction = resid
        norm_now = jnp.sum(resid * resid, axis=1)
        for step in range(CG_STEPS):
            image = direction + apply_cols(apply_rows(direction, matrix), matrix)
            alpha = norm_now / jnp.sum(direction * image, axis=1)
            coeffs = coeffs + alpha[:, None] * direction
            resid = resid - alpha[:, None] * image
            if step + 1 < CG_STEPS:
                norm_next = jnp.sum(resid * resid, axis=1)
                direction = resid + (norm_next / norm_now)[:, None] * direction
                norm_now = norm_next
        target = apply_rows(coeffs, matrix) + margin_dual
        margins = proximal(target, sign[None, :])
        margin_dual = target - margins
        total = coeffs + dual
        sparse = jnp.sign(total) * jnp.maximum(jnp.abs(total) - lambdas[:, None], 0.0)
        dual = total - sparse
    return coeffs, sparse, margins, margin_dual
```

```python
import functools

import jax
import jax.numpy as jnp
from jax import lax
from jax.experimental import pallas as pl
from jax.experimental.pallas import tpu as pltpu
from jax.sharding import PartitionSpec as P

ITERS = 2
CG_STEPS = 5
NEWTON_STEPS = 8
LANES = 128
ROW_TILE = 256
COL_TILE = 512
KERNEL_VMEM = 14 * 2**20


f32 = jnp.float32
bf16 = jnp.bfloat16
VM = pl.BlockSpec(memory_space=pltpu.VMEM)


def call(body, outs, args, name, weights=0, flops=0, **kw):
    args = list(args)
    for i in range(len(args) - weights, len(args)):
        args[i] = pltpu.with_memory_space_constraint(args[i], pltpu.VMEM)
    moved = sum(a.size * a.dtype.itemsize for a in args)
    return pl.pallas_call(
        body,
        in_specs=[VM] * len(args),
        out_specs=[VM] * len(outs),
        out_shape=[jax.ShapeDtypeStruct(s, f32) for s in outs],
        name=name,
        compiler_params=pltpu.CompilerParams(vmem_limit_bytes=KERNEL_VMEM),
        cost_estimate=pl.CostEstimate(flops=flops, bytes_accessed=moved, transcendentals=0),
        **kw,
    )(*args)


def parts_of(x):
    hi = x.astype(bf16)
    return hi, (x - hi.astype(f32)).astype(bf16)


def prep_kernel(m_ref, hi, lo, t_hi, t_lo):
    tile = m_ref.shape[0]
    rows = pl.ds(pl.multiple_of(pl.program_id(0) * tile, tile), tile)
    h, l = parts_of(m_ref[...])
    hi[rows, :] = h
    lo[rows, :] = l
    t_hi[:, rows] = h.T
    t_lo[:, rows] = l.T


def prep(matrix):
    n, k = matrix.shape
    tile = min(ROW_TILE, n)
    return pl.pallas_call(
        prep_kernel,
        grid=(n // tile,),
        in_specs=[pl.BlockSpec((tile, k), lambda i: (i, 0))],
        out_specs=[VM] * 4,
        out_shape=[
            pltpu.VMEM((n, k), bf16),
            pltpu.VMEM((n, k), bf16),
            pltpu.VMEM((k, n), bf16),
            pltpu.VMEM((k, n), bf16),
        ],
        name="prep",
        compiler_params=pltpu.CompilerParams(vmem_limit_bytes=KERNEL_VMEM),
    )(matrix)


def stacked(x):
    return jnp.concatenate(parts_of(x), 0)


def product(lhs, hi, lo, cols):
    acc = jnp.dot(lhs, hi[:, cols], preferred_element_type=f32)
    acc = acc + jnp.dot(lhs, lo[:, cols], preferred_element_type=f32)
    m = lhs.shape[0] // 2
    return acc[:m] + acc[m:]


def span(j, n):
    return pl.ds(pl.multiple_of(j * n, n), n)


def row_sum(x):
    return jnp.sum(x, axis=1, keepdims=True)


def wide(x):
    return jnp.broadcast_to(x, (x.shape[0], LANES))


def tree(items):
    if len(items) == 1:
        return items[0]
    h = len(items) // 2
    return tree(items[:h]) + tree(items[h:])


def xor_perm(x, axis, size, k):
    return lax.ppermute(x, axis, [(i, i ^ k) for i in range(size)])


def local(rows_n, cols_n, matrix, labels, lambdas, x_prev, w_prev, p_prev, z_prev, u_prev):
    paths, nf = x_prev.shape
    ns = z_prev.shape[1]
    fc = nf // rows_n
    half = ns // 2
    tile = min(COL_TILE, half)
    mm_flops = 2 * 4 * paths * nf * ns
    hi, lo, t_hi, t_lo = prep(matrix)
    full_f, full_s, chunk, one = (paths, nf), (paths, ns), (paths, fc), (paths, LANES)
    sent = (paths, fc + LANES)
    split = (paths, half + LANES)

    def scatter_rows(pieces):
        return [pieces[0]] + [xor_perm(pieces[k], "rows", rows_n, k) for k in range(1, rows_n)]

    def gather_rows(piece):
        return [piece] + [xor_perm(piece, "rows", rows_n, k) for k in range(1, rows_n)]

    def sum_cols(other, own):
        s = own + xor_perm(other, "cols", cols_n, 1)
        k = 2
        while k < cols_n:
            s = s + xor_perm(s, "cols", cols_n, k)
            k *= 2
        return s, xor_perm(s[:, :half], "cols", cols_n, 1)

    def write_halves(lhs, th, tl, other_ref, own_ref, scal):
        core = lax.rem(lax.axis_index("cols"), 2)
        for ref, h in ((other_ref, 1 - core), (own_ref, core)):
            for j in range(half // tile):
                cols = pl.ds(pl.multiple_of(h * half + j * tile, tile), tile)
                ref[:, j * tile : (j + 1) * tile] = product(lhs, th, tl, cols)
            ref[:, half:] = scal

    def fwd_first_kernel(x_ref, th, tl, other_ref, own_ref):
        write_halves(stacked(x_ref[...]), th, tl, other_ref, own_ref, jnp.zeros(one, f32))

    def fwd_kernel(first, *refs):
        got = refs[:rows_n]
        refs = refs[rows_n:]
        d_old = None
        if not first:
            d_old, refs = refs[0], refs[1:]
        th, tl, other_ref, own_ref, r_ref = refs
        me = lax.axis_index("rows")
        for k in range(rows_n):
            r_ref[:, span(me ^ k, fc)] = got[k][...]
        r = r_ref[...]
        rr = row_sum(r * r)
        rd = jnp.zeros_like(rr) if first else row_sum(r * d_old[...])
        lane = lax.broadcasted_iota(jnp.int32, one, 1)
        scal = jnp.where(lane < LANES // 2, wide(rr), wide(rd))
        write_halves(stacked(r), th, tl, other_ref, own_ref, scal)

    def join(own_ref, got_ref, out_ref):
        core = lax.rem(lax.axis_index("cols"), 2)
        out_ref[:, span(core, half)] = own_ref[:, :half]
        out_ref[:, span(1 - core, half)] = got_ref[...]

    def write_pieces(v, scal, h_ref, l_ref, pieces):
        me = lax.axis_index("rows")
        lhs = stacked(v)
        for k in range(rows_n - 1, -1, -1):
            pieces[k][:, :fc] = product(lhs, h_ref, l_ref, span(me ^ k, fc))
            pieces[k][:, fc:] = scal

    def direction_step(first, refs):
        if first:
            own, got, r_ref, ad_ref, d_ref, rr_ref, dd_ref = refs
        else:
            own, got, r_ref, ad_old, d_old, rr_old, dd_old, ad_ref, d_ref, rr_ref, dd_ref = refs
        join(own, got, ad_ref)
        rr = own[:, half : half + 1]
        if first:
            dd = rr
            d_ref[...] = r_ref[...]
            ad = ad_ref[...]
        else:
            rd = own[:, half + LANES // 2 : half + LANES // 2 + 1]
            beta = rr / rr_old[:, :1]
            dd = rr + 2.0 * beta * rd + beta * beta * dd_old[:, :1]
            d_ref[...] = r_ref[...] + beta * d_old[...]
            ad = ad_ref[...] + beta * ad_old[...]
            ad_ref[...] = ad
        rr_ref[...] = wide(rr)
        dd_ref[...] = wide(dd)
        return ad, row_sum(ad * ad)

    def bwd_kernel(first, *refs):
        n_in = 3 if first else 7
        ins, (h_ref, l_ref), outs = refs[:n_in], refs[n_in : n_in + 2], refs[n_in + 2 :]
        ad, sq = direction_step(first, tuple(ins) + tuple(outs[:4]))
        write_pieces(ad, wide(sq), h_ref, l_ref, outs[4:])

    def last_kernel(*refs):
        ad, sq = direction_step(False, refs[:-1])
        refs[-1][...] = wide(sq)

    def alpha_of(rr_ref, dd_ref, sq):
        return rr_ref[:, :1] / (dd_ref[:, :1] + sq)

    def update_kernel(*refs):
        got = refs[:rows_n]
        d_ref, r_ref, rr_ref, dd_ref, out_ref, alpha_ref = refs[rows_n:]
        me = lax.axis_index("rows")
        t = tree([g[...] for g in got])
        alpha = alpha_of(rr_ref, dd_ref, t[:, fc : fc + 1])
        mine = span(me, fc)
        out_ref[...] = r_ref[:, mine] - alpha * (d_ref[:, mine] + t[:, :fc])
        alpha_ref[...] = wide(alpha)

    def accumulate_kernel(alpha_ref, d_ref, ad_ref, x_ref, ax_ref, x_out, ax_out):
        alpha = alpha_ref[:, :1]
        x_out[...] = x_ref[...] + alpha * d_ref[...]
        ax_out[...] = ax_ref[...] + alpha * ad_ref[...]

    def start_kernel(*refs):
        got = refs[:rows_n]
        w_ref, p_ref, x_ref, out_ref = refs[rows_n:]
        mine = span(lax.axis_index("rows"), fc)
        t = tree([g[:, :fc] for g in got])
        out_ref[...] = (w_ref[:, mine] - p_ref[:, mine] - x_ref[:, mine]) + t

    def begin_kernel(own, got, z_ref, u_ref, h_ref, l_ref, ax_ref, *pieces):
        join(own, got, ax_ref)
        v = z_ref[...] - u_ref[...] - ax_ref[...]
        write_pieces(v, jnp.zeros(one, f32), h_ref, l_ref, pieces)

    def prox(target, sign):
        m = target
        for _ in range(NEWTON_STEPS):
            s = jax.nn.sigmoid(m)
            c = jax.nn.sigmoid(-m)
            grad = m - target - sign * jnp.where(sign > 0, c, s)
            m = m - grad / (1.0 + s * c)
        return m

    def finish(refs):
        sqs = refs[:rows_n]
        rr, dd, d, ad, x, ax, u, sign, x_out, ax_out, z_out, u_out = refs[rows_n:]
        alpha = alpha_of(rr, dd, tree([s[...] for s in sqs])[:, :1])
        x_out[...] = x[...] + alpha * d[...]
        ax_out[...] = ax[...] + alpha * ad[...]
        sg = sign[...]
        def one_tile(j, _):
            cols = span(j, LANES)
            target = ax_out[:, cols] + u[:, cols]
            m = prox(target, sign[:, cols])
            z_out[:, cols] = m
            u_out[:, cols] = target - m
            return 0
        lax.fori_loop(0, ns // LANES, one_tile, 0)

    def finish_kernel(*refs):
        finish(refs)

    def finish_bwd_kernel(*refs):
        n_in = rows_n + 8
        ins, (h_ref, l_ref), outs = refs[:n_in], refs[n_in : n_in + 2], refs[n_in + 2 :]
        finish(tuple(ins) + tuple(outs[:4]))
        ax, z, u = outs[1], outs[2], outs[3]
        v = z[...] - u[...] - ax[...]
        write_pieces(v, jnp.zeros(one, f32), h_ref, l_ref, outs[4:])

    def sparse_kernel(x_ref, p_ref, lam_ref, w_out, p_out):
        total = x_ref[...] + p_ref[...]
        mag = jnp.maximum(jnp.abs(total) - lam_ref[:, :1], 0.0)
        sgn = jnp.where(total > 0.0, 1.0, jnp.where(total < 0.0, -1.0, 0.0))
        w = sgn * mag
        w_out[...] = w
        p_out[...] = total - w

    sign = jnp.broadcast_to((2.0 * labels.astype(f32) - 1.0)[None, :], (8, ns))
    sign = jnp.tile(sign, (paths // 8, 1))
    lam = jnp.broadcast_to(lambdas[:, None], one)

    x, w, p, z, u = x_prev, w_prev, p_prev, z_prev, u_prev
    other, own = call(fwd_first_kernel, [split] * 2, (x, t_hi, t_lo), "fwd0", 2, mm_flops)
    own, got = sum_cols(other, own)
    ax, *pieces = call(
        begin_kernel, [full_s] + [sent] * rows_n, (own, got, z, u, hi, lo), "begin", 2, mm_flops
    )
    for outer in range(ITERS):
        pieces = scatter_rows(pieces)
        (r_chunk,) = call(start_kernel, [chunk], (*pieces, w, p, x), "start")
        d = ad = rr = dd = None
        for step in range(CG_STEPS):
            first = step == 0
            r_parts = gather_rows(r_chunk)
            if not first:
                x, ax = call(
                    accumulate_kernel, [full_f, full_s], (alpha, d, ad, x, ax), "accumulate"
                )
            extra = () if first else (d,)
            other, own, r = call(
                functools.partial(fwd_kernel, first),
                [split, split, full_f],
                (*r_parts, *extra, t_hi, t_lo),
                "fwd",
                2,
                mm_flops,
            )
            own, got = sum_cols(other, own)
            olds = () if first else (ad, d, rr, dd)
            outs = [full_s, full_f, one, one]
            if step + 1 < CG_STEPS:
                ad, d, rr, dd, *pieces = call(
                    functools.partial(bwd_kernel, first),
                    outs + [sent] * rows_n,
                    (own, got, r, *olds, hi, lo),
                    "bwd",
                    2,
                    mm_flops,
                )
                pieces = scatter_rows(pieces)
                r_chunk, alpha = call(
                    update_kernel, [chunk, one], (*pieces, d, r, rr, dd), "update"
                )
            else:
                ad, d, rr, dd, sq = call(last_kernel, outs + [one], (own, got, r, *olds), "last")
                sqs = gather_rows(sq)
        ins = (*sqs, rr, dd, d, ad, x, ax, u, sign)
        outs = [full_f, full_s, full_s, full_s]
        if outer + 1 < ITERS:
            x, ax, z, u, *pieces = call(
                finish_bwd_kernel, outs + [sent] * rows_n, (*ins, hi, lo), "finish", 2, mm_flops
            )
        else:
            x, ax, z, u = call(finish_kernel, outs, ins, "finish")
        w, p = call(sparse_kernel, [full_f, full_f], (x, p, lam), "sparse")
    return x, w, z, u


def solution(mesh):
    return jax.shard_map(
        functools.partial(local, mesh.shape["rows"], mesh.shape["cols"]),
        mesh=mesh,
        in_specs=(
            P(("rep", "rows"), "cols"),
            P(("rep", "rows")),
            P("rep"),
            P("rep", "cols"),
            P("rep", "cols"),
            P("rep", "cols"),
            P("rep", "rows"),
            P("rep", "rows"),
        ),
        out_specs=(P("rep", "cols"), P("rep", "cols"), P("rep", "rows"), P("rep", "rows")),
        check_vma=False,
    )
```

```python
import functools

import jax
import jax.numpy as jnp
from jax import lax
from jax.experimental import pallas as pl
from jax.experimental.pallas import tpu as pltpu
from jax.sharding import PartitionSpec as P

ITERS = 2
CG_STEPS = 5
NEWTON_STEPS = 8
LANES = 128
SUBLANES = 8
ROW_TILE = 256
COL_TILE = 512
KERNEL_VMEM = 6 * 2**20
PREP_VMEM = 10 * 2**20


f32 = jnp.float32
bf16 = jnp.bfloat16
VM = pl.BlockSpec(memory_space=pltpu.VMEM)


def call(body, outs, args, weights=0, flops=0):
    args = list(args)
    for i in range(len(args) - weights, len(args)):
        args[i] = pltpu.with_memory_space_constraint(args[i], pltpu.VMEM)
    moved = sum(a.size * a.dtype.itemsize for a in args)
    return pl.pallas_call(
        body,
        in_specs=[VM] * len(args),
        out_specs=[VM] * len(outs),
        out_shape=[jax.ShapeDtypeStruct(s, f32) for s in outs],
        compiler_params=pltpu.CompilerParams(vmem_limit_bytes=KERNEL_VMEM),
        cost_estimate=pl.CostEstimate(flops=flops, bytes_accessed=moved, transcendentals=0),
    )(*args)


def parts_of(x):
    hi = x.astype(bf16)
    return hi, (x - hi.astype(f32)).astype(bf16)


def stacked(x):
    return jnp.concatenate(parts_of(x), 0)


def product(lhs, hi, lo, rows, cols):
    acc = jnp.dot(lhs, hi[rows, cols], preferred_element_type=f32)
    return acc + jnp.dot(lhs, lo[rows, cols], preferred_element_type=f32)


def folded(acc):
    m = acc.shape[0] // 2
    return acc[:m] + acc[m:]


def span(j, n):
    return pl.ds(pl.multiple_of(j * n, n), n)


def row_sum(x):
    return jnp.sum(x, axis=1, keepdims=True)


def wide(x):
    return jnp.broadcast_to(x, (x.shape[0], LANES))


def put_blocks(ref, value, at=0):
    m = value.shape[0]
    for j in range(value.shape[1] // LANES):
        ref[at + j * m : at + (j + 1) * m, :] = value[:, j * LANES : (j + 1) * LANES]


def get_blocks(value, m, n):
    return jnp.concatenate([value[j * m : (j + 1) * m, :] for j in range(n // LANES)], 1)


def pack(columns):
    groups = columns[0].shape[0] // SUBLANES
    width = LANES // (groups * len(columns))
    slot = lax.broadcasted_iota(jnp.int32, (SUBLANES, LANES), 1) // width
    tile = jnp.zeros((SUBLANES, LANES), f32)
    for i, c in enumerate(columns):
        for a in range(groups):
            part = wide(c[a * SUBLANES : (a + 1) * SUBLANES])
            tile = jnp.where(slot == i * groups + a, part, tile)
    return tile


def unpack(tile, paths, i, n):
    groups = paths // SUBLANES
    width = LANES // (groups * n)
    at = [(i * groups + a) * width for a in range(groups)]
    return jnp.concatenate([tile[:, c : c + 1] for c in at], 0)


def tree(items):
    if len(items) == 1:
        return items[0]
    h = len(items) // 2
    return tree(items[:h]) + tree(items[h:])


def send_order(rows_n):
    return [k for k in (*range(rows_n // 2, rows_n), *range(1, rows_n // 2)) if k > 0]


def xor_perm(x, axis, size, k):
    return lax.ppermute(x, axis, [(i, i ^ k) for i in range(size)])


def prep_kernel(m_ref, x_ref, hi, lo, t_hi, t_lo, u_ref):
    tile = m_ref.shape[0]
    paths = x_ref.shape[0]
    step = pl.program_id(0)
    rows = span(step, tile)
    h, l = parts_of(m_ref[...])
    hi[rows, :] = h
    lo[rows, :] = l
    ht, lt = h.T, l.T
    t_hi[:, rows] = ht
    t_lo[:, rows] = lt
    lhs = stacked(x_ref[...])
    acc = jnp.dot(lhs, ht, preferred_element_type=f32)
    u = folded(acc + jnp.dot(lhs, lt, preferred_element_type=f32))
    blocks = tile // LANES
    core = lax.rem(lax.axis_index("cols"), 2)
    per_half = pl.num_programs(0) // 2
    place = lax.rem(step + core * per_half, 2 * per_half)
    for j in range(blocks):
        u_ref[span(place * blocks + j, paths), :] = u[:, j * LANES : (j + 1) * LANES]


def prep(matrix, x):
    n, k = matrix.shape
    tile = min(ROW_TILE, n // 2)
    paths = x.shape[0]
    return pl.pallas_call(
        prep_kernel,
        grid=(n // tile,),
        in_specs=[pl.BlockSpec((tile, k), lambda i: (i, 0)), VM],
        out_specs=[VM] * 5,
        out_shape=[
            pltpu.VMEM((n, k), bf16),
            pltpu.VMEM((n, k), bf16),
            pltpu.VMEM((k, n), bf16),
            pltpu.VMEM((k, n), bf16),
            jax.ShapeDtypeStruct((paths * n // LANES, LANES), f32),
        ],
        name="prep",
        compiler_params=pltpu.CompilerParams(vmem_limit_bytes=PREP_VMEM),
    )(matrix, x)


def prox(target, sign):
    m = target
    for _ in range(NEWTON_STEPS):
        e = jnp.exp(-jnp.abs(m))
        big = 1.0 / (1.0 + e)
        small = e * big
        pull = jnp.where((m >= 0.0) == (sign > 0.0), small, big)
        m = m - (m - target - sign * pull) / (1.0 + big * small)
    return m


def local(rows_n, cols_n, matrix, labels, lambdas, x_prev, w_prev, p_prev, z_prev, u_prev):
    paths, nf = x_prev.shape
    ns = z_prev.shape[1]
    fc = nf // rows_n
    half = ns // 2
    tile = min(COL_TILE, half)
    work = 2 * 4 * paths * nf * ns
    full_f, full_s, chunk, one = (paths, nf), (paths, ns), (paths, fc), (paths, LANES)
    scal = (SUBLANES, LANES)
    top = paths * fc // LANES
    mid = paths * half // LANES
    piece = (top + SUBLANES, LANES)
    split = (mid + SUBLANES, LANES)
    order = send_order(rows_n)
    early, late = list(range(max(rows_n // 2, 1))), list(range(max(rows_n // 2, 1), rows_n))
    ahead, behind = order[:2], order[2:] + [0]

    def send_rows(values):
        got = {}
        for k in order:
            got[k] = xor_perm(values[k], "rows", rows_n, k)
        return got

    def sum_cols(other, own):
        s = own + xor_perm(other, "cols", cols_n, 1)
        k = 2
        while k < cols_n:
            s = s + xor_perm(s, "cols", cols_n, k)
            k *= 2
        return s, xor_perm(s, "cols", cols_n, 1)

    def core_half():
        return lax.rem(lax.axis_index("cols"), 2)

    def fwd_early_kernel(*refs):
        got, (th, tl, acc_ref) = refs[:-3], refs[-3:]
        me = lax.axis_index("rows")
        lhs = [stacked(g[...]) for g in got]

        @pl.loop(0, ns // tile)
        def _(j):
            cols = span(j, tile)
            acc = [product(v, th, tl, span(me ^ k, fc), cols) for v, k in zip(lhs, early)]
            acc_ref[:, cols] = folded(sum(acc[1:], acc[0]))

    def fwd_half(h, got, acc_ref, th, tl, out_ref):
        me = lax.axis_index("rows")
        lhs = [stacked(g[...]) for g in got]

        @pl.loop(0, half // tile)
        def _(j):
            cols = pl.ds(pl.multiple_of(h * half + j * tile, tile), tile)
            u = acc_ref[:, cols]
            acc = [product(v, th, tl, span(me ^ k, fc), cols) for v, k in zip(lhs, late)]
            if acc:
                u = u + folded(sum(acc[1:], acc[0]))
            for i in range(tile // LANES):
                rows = span(j * (tile // LANES) + i, paths)
                out_ref[rows, :] = u[:, i * LANES : (i + 1) * LANES]

    def fwd_other_kernel(first, *refs):
        got, refs = refs[:rows_n], refs[rows_n:]
        if not first:
            d_old, refs = refs[0], refs[1:]
        acc_ref, th, tl, out_ref, r_ref, scal_ref = refs
        me = lax.axis_index("rows")
        for g, k in zip(got, early + late):
            r_ref[:, span(me ^ k, fc)] = g[...]
        r = r_ref[...]
        rr = row_sum(r * r)
        rd = jnp.zeros_like(rr) if first else row_sum(r * d_old[...])
        scalars = pack([rr, rd])
        scal_ref[...] = scalars
        out_ref[mid:, :] = scalars
        fwd_half(1 - core_half(), got[len(early) :], acc_ref, th, tl, out_ref)

    def fwd_own_kernel(*refs):
        got, (scal_ref, acc_ref, th, tl, out_ref) = refs[:-5], refs[-5:]
        out_ref[mid:, :] = scal_ref[...]
        fwd_half(core_half(), got, acc_ref, th, tl, out_ref)

    def bwd_own_kernel(first, *refs):
        if first:
            own, r_ref, h_ref, l_ref, ad_ref, d_ref, rr_ref, dd_ref, acc_ref = refs
        else:
            own, r_ref, ad_old, d_old, rr_old, dd_old = refs[:6]
            h_ref, l_ref, ad_ref, d_ref, rr_ref, dd_ref, acc_ref = refs[6:]
        me, core = lax.axis_index("rows"), core_half()
        rr = unpack(own[mid:, :], paths, 0, 2)
        ad = get_blocks(own[...], paths, half)
        if first:
            dd = rr
            d_ref[...] = r_ref[...]
        else:
            rd = unpack(own[mid:, :], paths, 1, 2)
            beta = rr / rr_old[:, :1]
            dd = rr + 2.0 * beta * rd + beta * beta * dd_old[:, :1]
            d_ref[...] = r_ref[...] + beta * d_old[...]
            ad = ad + beta * ad_old[:, span(core, half)]
        ad_ref[...] = ad
        rr_ref[...] = wide(rr)
        dd_ref[...] = wide(dd)
        if acc_ref is None:
            return
        lhs = stacked(ad)

        @pl.loop(0, rows_n)
        def _(k):
            acc = product(lhs, h_ref, l_ref, span(core, half), span(me ^ k, fc))
            acc_ref[:, span(k, fc)] = folded(acc)

    def join_ad(first, got, own_ref, rr_ref, ad_old, rr_old, ad_ref):
        core = core_half()
        ad = get_blocks(got[...], paths, half)
        if not first:
            ad = ad + (rr_ref[:, :1] / rr_old[:, :1]) * ad_old[:, span(1 - core, half)]
        ad_ref[:, span(core, half)] = own_ref[...]
        ad_ref[:, span(1 - core, half)] = ad
        return ad

    def write_piece(ref, value, scalars):
        put_blocks(ref, value)
        ref[top:, :] = scalars

    def bwd_other(ks, ad, scalars, acc_ref, h_ref, l_ref, outs):
        me, core = lax.axis_index("rows"), core_half()
        lhs = stacked(ad)
        for k, ref in zip(ks, outs):
            acc = product(lhs, h_ref, l_ref, span(1 - core, half), span(me ^ k, fc))
            write_piece(ref, acc_ref[:, k * fc : (k + 1) * fc] + folded(acc), scalars)

    def bwd_ahead_kernel(first, *refs):
        got, own_ref, rr_ref = refs[:3]
        ad_old = rr_old = None
        refs = refs[3:]
        if not first:
            ad_old, rr_old = refs[:2]
            refs = refs[2:]
        acc_ref, h_ref, l_ref, ad_ref, scal_ref = refs[:5]
        ad = join_ad(first, got, own_ref, rr_ref, ad_old, rr_old, ad_ref)
        own = own_ref[...]
        scalars = pack([row_sum(own * own) + row_sum(ad * ad)])
        scal_ref[...] = scalars
        bwd_other(ahead, ad, scalars, acc_ref, h_ref, l_ref, refs[5:])

    def bwd_behind_kernel(ad_ref, scal_ref, acc_ref, h_ref, l_ref, *outs):
        ad = ad_ref[:, span(1 - core_half(), half)]
        bwd_other(behind, ad, scal_ref[...], acc_ref, h_ref, l_ref, outs)

    def last_kernel(got, own_ref, rr_ref, ad_old, rr_old, ad_ref, scal_ref):
        ad = join_ad(False, got, own_ref, rr_ref, ad_old, rr_old, ad_ref)
        own = own_ref[...]
        scal_ref[...] = pack([row_sum(own * own) + row_sum(ad * ad)])

    def whole_pieces(ks, v, h_ref, l_ref, outs):
        me = lax.axis_index("rows")
        lhs = stacked(v)
        for k, ref in zip(ks, outs):
            acc = product(lhs, h_ref, l_ref, slice(None), span(me ^ k, fc))
            write_piece(ref, folded(acc), jnp.zeros(scal, f32))

    def whole_behind_kernel(v_ref, h_ref, l_ref, *outs):
        whole_pieces(behind, v_ref[...], h_ref, l_ref, outs)

    def alpha_of(rr_ref, dd_ref, tile):
        return rr_ref[:, :1] / (dd_ref[:, :1] + unpack(tile, paths, 0, 1))

    def update_kernel(*refs):
        got = refs[:rows_n]
        d_ref, r_ref, rr_ref, dd_ref, out_ref, alpha_ref = refs[rows_n:]
        t = tree([g[...] for g in got])
        alpha = alpha_of(rr_ref, dd_ref, t[top:])
        mine = span(lax.axis_index("rows"), fc)
        image = d_ref[:, mine] + get_blocks(t, paths, fc)
        out_ref[...] = r_ref[:, mine] - alpha * image
        alpha_ref[...] = wide(alpha)

    def accumulate_kernel(alpha_ref, d_ref, ad_ref, x_ref, ax_ref, x_out, ax_out):
        alpha = alpha_ref[:, :1]
        x_out[...] = x_ref[...] + alpha * d_ref[...]
        ax_out[...] = ax_ref[...] + alpha * ad_ref[...]

    def start_kernel(*refs):
        got = refs[:rows_n]
        w_ref, p_ref, x_ref, out_ref = refs[rows_n:]
        mine = span(lax.axis_index("rows"), fc)
        t = get_blocks(tree([g[...] for g in got]), paths, fc)
        out_ref[...] = (w_ref[:, mine] - p_ref[:, mine] - x_ref[:, mine]) + t

    def begin_kernel(own, got, z_ref, u_ref, h_ref, l_ref, ax_ref, v_ref, *outs):
        core = core_half()
        ax_ref[:, span(core, half)] = get_blocks(own[...], paths, half)
        ax_ref[:, span(1 - core, half)] = get_blocks(got[...], paths, half)
        v = z_ref[...] - u_ref[...] - ax_ref[...]
        v_ref[...] = v
        whole_pieces(ahead, v, h_ref, l_ref, outs)

    def finish_kernel(final, *refs):
        sqs = refs[:rows_n]
        rr, dd, d, ad, x, ax, u, p, sign, lam = refs[rows_n : rows_n + 10]
        refs = refs[rows_n + 10 :]
        if not final:
            h_ref, l_ref = refs[:2]
            refs = refs[2:]
        x_out, ax_out, z_out, u_out, w_out, p_out = refs[:6]
        alpha = alpha_of(rr, dd, tree([s[...] for s in sqs]))
        x_new = x[...] + alpha * d[...]
        x_out[...] = x_new
        ax_out[...] = ax[...] + alpha * ad[...]

        @pl.loop(0, ns // tile)
        def _(j):
            cols = span(j, tile)
            target = ax_out[:, cols] + u[:, cols]
            m = prox(target, jnp.broadcast_to(sign[:1, cols], target.shape))
            z_out[:, cols] = m
            u_out[:, cols] = target - m

        total = x_new + p[...]
        mag = jnp.maximum(jnp.abs(total) - lam[:, :1], 0.0)
        w = jnp.where(total > 0.0, mag, jnp.where(total < 0.0, -mag, 0.0))
        w_out[...] = w
        p_out[...] = total - w
        if not final:
            v = z_out[...] - u_out[...] - ax_out[...]
            refs[6][...] = v
            whole_pieces(ahead, v, h_ref, l_ref, refs[7:])

    sign = jnp.broadcast_to((2.0 * labels.astype(f32) - 1.0)[None, :], (SUBLANES, ns))
    lam = jnp.broadcast_to(lambdas[:, None], one)

    x, w, p, z, u = x_prev, w_prev, p_prev, z_prev, u_prev
    hi, lo, t_hi, t_lo, blocks = prep(matrix, x)
    own, got = sum_cols(blocks[mid:], blocks[:mid])
    n_ahead, n_behind = [piece] * len(ahead), [piece] * len(behind)
    ax, v, *out = call(
        begin_kernel, [full_s, full_s] + n_ahead, (own, got, z, u, hi, lo), 2, work // 2
    )
    for outer in range(ITERS):
        sent = dict(zip(ahead, out))
        out = call(whole_behind_kernel, n_behind, (v, hi, lo), 2, work // 2)
        sent.update(zip(behind, out))
        pieces = {0: sent[0], **send_rows(sent)}
        pieces = [pieces[k] for k in range(rows_n)]
        (r_chunk,) = call(start_kernel, [chunk], (*pieces, w, p, x))
        for step in range(CG_STEPS):
            first = step == 0
            got = {0: r_chunk, **send_rows({k: r_chunk for k in order})}
            if not first:
                x, ax = call(accumulate_kernel, [full_f, full_s], (alpha, d, ad, x, ax))
            (acc,) = call(
                fwd_early_kernel, [full_s], (*[got[k] for k in early], t_hi, t_lo), 2,
                work // 2,
            )
            extra = () if first else (d,)
            other, r, scalars = call(
                functools.partial(fwd_other_kernel, first),
                [split, full_f, scal],
                (*[got[k] for k in early + late], *extra, acc, t_hi, t_lo),
                2,
                work // 4,
            )
            (own,) = call(
                fwd_own_kernel,
                [split],
                (*[got[k] for k in late], scalars, acc, t_hi, t_lo),
                2,
                work // 4,
            )
            own, got = sum_cols(other, own)
            olds = () if first else (ad, d, rr, dd)
            some = () if first else (ad, rr)
            outs = [(paths, half), full_f, one, one]
            if step + 1 < CG_STEPS:
                ad_own, d, rr, dd, acc = call(
                    functools.partial(bwd_own_kernel, first),
                    outs + [full_f],
                    (own, r, *olds, hi, lo),
                    2,
                    work // 2,
                )
                ad, scalars, *out = call(
                    functools.partial(bwd_ahead_kernel, first),
                    [full_s, scal] + n_ahead,
                    (got, ad_own, rr, *some, acc, hi, lo),
                    2,
                    work // 4,
                )
                sent = dict(zip(ahead, out))
                out = call(bwd_behind_kernel, n_behind, (ad, scalars, acc, hi, lo), 2, work // 4)
                sent.update(zip(behind, out))
                pieces = {0: sent[0], **send_rows(sent)}
                pieces = [pieces[k] for k in range(rows_n)]
                r_chunk, alpha = call(update_kernel, [chunk, one], (*pieces, d, r, rr, dd))
            else:
                ad_own, d, rr, dd = call(
                    lambda *refs: bwd_own_kernel(False, *refs[:6], None, None, *refs[6:], None),
                    outs,
                    (own, r, *olds),
                )
                ad, sq = call(last_kernel, [full_s, scal], (got, ad_own, rr, *some))
                sqs = {0: sq, **send_rows({k: sq for k in order})}
        ins = (*[sqs[k] for k in range(rows_n)], rr, dd, d, ad, x, ax, u, p, sign, lam)
        outs = [full_f, full_s, full_s, full_s, full_f, full_f]
        if outer + 1 < ITERS:
            x, ax, z, u, w, p, v, *out = call(
                functools.partial(finish_kernel, False),
                outs + [full_s] + n_ahead,
                (*ins, hi, lo),
                2,
                work // 2,
            )
        else:
            x, ax, z, u, w, p = call(functools.partial(finish_kernel, True), outs, ins)
    return x, w, z, u


def solution(mesh):
    return jax.shard_map(
        functools.partial(local, mesh.shape["rows"], mesh.shape["cols"]),
        mesh=mesh,
        in_specs=(
            P(("rep", "rows"), "cols"),
            P(("rep", "rows")),
            P("rep"),
            P("rep", "cols"),
            P("rep", "cols"),
            P("rep", "cols"),
            P("rep", "rows"),
            P("rep", "rows"),
        ),
        out_specs=(P("rep", "cols"), P("rep", "cols"), P("rep", "rows"), P("rep", "rows")),
        check_vma=False,
    )
```
